32 devices in a mesh: gz: 32 (over z, y, x, core).
Axes of the slice: x: 2, y: 2, z: 4, core: 2. Of those that a mesh axis runs over, the one named last changes fastest.
Arguments:
- velocity: float32 [3, 128, 256, 512], P(None, 'gz'), may hold values from -0.3 to 0.3
- offsets: float32 [3, 16384], P(None, 'gz'), may hold values from 1.2 to 1.8
- bases: int32 [3, 16384], P(None, 'gz'), may hold values from 0 to 511, as said below
- targets: float32 [3, 16384], P(None, 'gz'), may hold values from 1 to 2
- stiffness: float32 [16384], P('gz'), may hold values from 10 to 100
- active_block_count: int32 [32], P('gz'), may hold values from 1 to 2, as said below
Outputs:
- velocity_out: float32 [3, 128, 256, 512], P(None, 'gz')
- offsets_out: float32 [3, 16384], P(None, 'gz')
The draws below stay inside these ranges and needn't reach their ends.
Inputs may be any that keep to these rules, and one draw needn't show every extreme that they name: `bases`: rows are x, y, z. x lies in 0..511 and y in 0..255; the z of marker m lies in the slab of index m // 512, from (m // 512) * 4 to (m // 512) * 4 + 3. `active_block_count`: in every draw some slab uses all 2 blocks.
All inputs are finite; a program needn't handle non-finite values.
Results may differ from the reference program's by a relative error of at most 0.0015.
Values may be sent and summed in bfloat16 or wider, within the bound.
A program may use at most 192 MiB of HBM per device.

```python
import math
import jax
import jax.numpy as jnp
from jax import lax

NX = 512
NY = 256
CZ = 4
M_DEV = 512
BLK = 256
STEPS = 2
NBLK = 2
NZ = 128
MARKERS = 16384
SLABS = 32


def draw_bases(key, part):
    first_key, second_key, third_key = jax.random.split(key, 3)
    x_cells = jax.random.randint(first_key, (MARKERS,), 0, NX)
    y_cells = jax.random.randint(second_key, (MARKERS,), 0, NY)
    owners = jnp.arange(MARKERS, dtype=jnp.int32) // M_DEV
    z_cells = owners * CZ + jax.random.randint(third_key, (MARKERS,), 0, CZ)
    return jnp.stack([x_cells, y_cells, z_cells]).astype(jnp.int32)


def draw_active_block_count(key, part):
    count_key, chosen_key = jax.random.split(key)
    counts = jax.random.randint(count_key, (SLABS,), 1, NBLK + 1)
    chosen = jax.random.randint(chosen_key, (), 0, SLABS)
    return counts.at[chosen].set(NBLK).astype(jnp.int32)


def block_levels(own_key, extent, cuts, low, largest):
    def one(dim, parts):
        heights = jax.random.uniform(jax.random.fold_in(jax.random.fold_in(own_key, 6), dim), (parts,), jnp.float32, low / len(cuts), largest / len(cuts))
        return jnp.repeat(jnp.exp(heights), extent[dim] // parts).reshape((-1,) + (1,) * (len(extent) - dim - 1))

    level = one(*cuts[0])
    for cut in cuts[1:]:
        level = level * one(*cut)
    return level


def bell_draw(own_key, extent, width, bound, pieces=(), held_as=jnp.bfloat16):
    drawn = jax.random.normal(own_key, extent, jnp.float32) * width
    if len(pieces) > 0:
        drawn = block_levels(own_key, extent, pieces, -0.22, 0.18) * drawn
    return jnp.clip(drawn, min=-bound, max=bound).astype(held_as)


def setup_inputs(seed: int = 0) -> dict:
    keys = jax.random.split(jax.random.key(seed), 7)
    return {
        "velocity": bell_draw(keys[0], (3, NZ, NY, NX), 0.1, 0.3, ((1, 32),), jnp.float32),
        "offsets": jnp.clip(1.2 + 0.5999999 * jax.random.uniform(keys[1], (3, MARKERS), jnp.float32) ** block_levels(keys[1], (3, MARKERS), ((1, 32),), -0.2, 0.2), 1.2, 1.8),
        "bases": draw_bases(jax.random.fold_in(keys[6], 71), 0),
        "targets": jnp.clip(1.0 + 1.0 * jax.random.uniform(keys[3], (3, MARKERS), jnp.float32) ** block_levels(keys[3], (3, MARKERS), ((1, 32),), -0.2, 0.2), 1.0, 2.0),
        "stiffness": jnp.clip(jnp.exp(math.log(100.0) - 2.3025851 * jax.random.uniform(keys[4], (MARKERS,), jnp.float32) ** block_levels(keys[4], (MARKERS,), ((0, 32),), -0.2, 0.2)), 10.0, 100.0),
        "active_block_count": draw_active_block_count(jax.random.fold_in(keys[6], 71), 0),
    }


def kernel(offsets):
    steps_back = jnp.arange(4).astype(jnp.float32)
    return 0.25 * (1.0 + jnp.cos((0.5 * math.pi) * (offsets[:, None, :] - steps_back[None, :, None])))


def advance(velocity, forcing):
    laplace = -6.0 * velocity
    transport_velocity = jnp.zeros_like(velocity)
    for sweep_sense in (1, 2, 3):
        upper_cells = jnp.roll(velocity, -1, sweep_sense)
        lower_cells = jnp.roll(velocity, 1, sweep_sense)
        transfer_buffer = 3 - sweep_sense
        laplace = laplace + upper_cells + lower_cells
        transport_velocity = transport_velocity + velocity[transfer_buffer][None] * (upper_cells - lower_cells) * 0.5
    return velocity + 0.2 * (0.3 * laplace - transport_velocity + forcing)


def rounded(values):
    return lax.optimization_barrier(values.astype(jnp.bfloat16)).astype(jnp.float32)


def reference(velocity, offsets, bases, targets, stiffness, active_block_count):
    markers = offsets.shape[1]
    ordinal = jnp.arange(markers, dtype=jnp.int32)
    living = ((ordinal % M_DEV) // BLK < active_block_count[ordinal // M_DEV]).astype(jnp.float32)
    reach = jnp.arange(4, dtype=jnp.int32)
    xcells = (bases[0][None, :] + reach[:, None]) % NX
    ycells = (bases[1][None, :] + reach[:, None]) % NY
    zcells = (bases[2][None, :] + reach[:, None]) % NZ
    shape_all = (4, 4, 4, markers)
    z_index = jnp.broadcast_to(zcells[:, None, None, :], shape_all).reshape(-1)
    y_index = jnp.broadcast_to(ycells[None, :, None, :], shape_all).reshape(-1)
    x_index = jnp.broadcast_to(xcells[None, None, :, :], shape_all).reshape(-1)
    for step_number in range(STEPS):
        weights = kernel(offsets)
        forces = living[None, :] * stiffness[None, :] * (targets - offsets)
        vertical = rounded((forces[:, None, None, :] * weights[2][None, :, None, :]) * weights[1][None, None, :, :])
        across = rounded(weights[0])
        amounts = vertical[:, :, :, None, :] * across[None, None, None, :, :]
        forcing = jnp.zeros_like(velocity).at[:, z_index, y_index, x_index].add(amounts.reshape(3, -1))
        velocity = advance(velocity, forcing)
        lowered = velocity.astype(jnp.bfloat16)
        picked = lowered[:, z_index, y_index, x_index].astype(jnp.float32).reshape(3, 4, 4, 4, markers)
        mixed = rounded(weights[2][:, None, :] * weights[1][None, :, :])
        sampled = jnp.sum((mixed[None, :, :, None, :] * picked) * weights[0][None, None, None, :, :], axis=(1, 2, 3))
        offsets = offsets + 0.2 * (living[None, :] * sampled)
    return velocity, offsets
```

```python
import functools
import math

import jax
import jax.numpy as jnp
from jax import lax
from jax.experimental import pallas as pl
from jax.experimental.pallas import tpu as pltpu
from jax.sharding import PartitionSpec as P

BLK = 256
STEPS = 2
DT = 0.2
VISC = 0.3
ROWS = 16


def shifted(value, steps):
    count = lax.axis_size("gz")
    pairs = [(source, (source + steps) % count) for source in range(count)]
    return lax.ppermute(value, "gz", pairs)


def joined(own_ref, near_ref, moved, layers):
    halves = []
    for ref, pair in ((own_ref, moved[:2]), (near_ref, moved[2:])):
        rows = ref[...]
        offsets = rows[0:3]
        if pair:
            sampled = pair[0][0:3, :] + pair[1][0:3, :]
            offsets = offsets + DT * (rows[9:10] * sampled)
        level = rows[5:6] if ref is own_ref else rows[5:6] - float(layers)
        forces = rows[10:11] * (rows[6:9] - offsets)
        halves.append((offsets, rows[3:5].astype(jnp.int32), level.astype(jnp.int32), forces))
    return [jnp.concatenate(parts, axis=1) for parts in zip(*halves)]


def weights_of(offsets):
    return [0.25 * (1.0 + jnp.cos((0.5 * math.pi) * (offsets - float(j)))) for j in range(4)]


def wrapped(cell, extent):
    return jnp.where(cell >= extent, cell - extent, cell)


def banded(across, cell, weights, extent):
    table = jnp.zeros(across.shape, jnp.float32)
    for j in range(4):
        table = jnp.where(across == wrapped(cell + j, extent), weights[j], table)
    return table


def plane_weights(level, weights_z, layers):
    planes = []
    for z in range(layers):
        row = jnp.zeros(level.shape, jnp.float32)
        for j in range(4):
            row = jnp.where(level + j == z, weights_z[j], row)
        planes.append(row)
    return planes


def columns_of(rows):
    pad = -len(rows) % 8
    zero = jnp.zeros_like(rows[0])
    return jnp.concatenate(rows + [zero] * pad, axis=0).T


def fill_xtable(table_ref, col_ref, first, low, extent, chunk):
    def body(i, _):
        r = pl.ds(i * chunk, chunk)
        cols = col_ref[r, :]
        across = lax.broadcasted_iota(jnp.int32, (chunk, extent), 1)
        cell = cols[:, first : first + 1].astype(jnp.int32)
        ws = [cols[:, first + 1 + j : first + 2 + j] for j in range(4)]
        table_ref[r, :] = banded(across, cell, ws, extent).astype(low)
        return 0

    lax.fori_loop(0, table_ref.shape[0] // chunk, body, 0)


def spread_kernel(layers, n_moved, *refs):
    own_ref, near_ref = refs[:2]
    moved = refs[2 : 2 + n_moved]
    v_hbm, p_hbm = refs[2 + n_moved : 4 + n_moved]
    vbuf, obuf, force, lhs, xtab, ytab, col, rowg, in_sem, out_sem = refs[4 + n_moved :]
    ny, nx = vbuf.shape[2], vbuf.shape[3]
    both = xtab.shape[0]

    load = pltpu.make_async_copy(v_hbm, vbuf, in_sem)
    load.start()

    offsets, cells, level, forces = joined(own_ref, near_ref, moved, layers)
    weights = weights_of(offsets)
    col[...] = columns_of(
        [cells[0:1].astype(jnp.float32)] + [w[0:1] for w in weights]
    )
    planes = plane_weights(level, [w[2:3] for w in weights], layers)
    for z in range(layers):
        rowg[z] = jnp.concatenate([forces * planes[z], jnp.zeros((5, both), jnp.float32)], axis=0)
    fill_xtable(xtab, col, 0, jnp.bfloat16, nx, 64)

    wy = [w[1:2] for w in weights]

    def ybody(i, _):
        across = lax.broadcasted_iota(jnp.int32, (8, both), 0) + i * 8
        ytab[pl.ds(i * 8, 8), :] = banded(across, cells[1:2], wy, ny)
        return 0

    lax.fori_loop(0, ny // 8, ybody, 0)
    load.wait()

    def plane(z, _):
        def lhs_body(i, _):
            y = ytab[pl.ds(i * 16, 16), :]
            for c in range(3):
                lhs[pl.ds(c * ny + i * 16, 16), :] = (rowg[z, c : c + 1, :] * y).astype(jnp.bfloat16)
            return 0

        lax.fori_loop(0, ny // 16, lhs_body, 0)
        force[...] = jnp.dot(lhs[...], xtab[...], preferred_element_type=jnp.float32)

        below = jnp.maximum(z - 1, 0)
        above = jnp.minimum(z + 1, layers - 1)
        has_below = jnp.where(z > 0, 1.0, 0.0)
        has_above = jnp.where(z < layers - 1, 1.0, 0.0)

        def stencil(i, _):
            n = 16
            y0 = i * n
            prev = jnp.where(i == 0, ny - 8, y0 - 8)
            nxt = jnp.where(y0 + n == ny, 0, y0 + n)
            here = [vbuf[c, z, pl.ds(y0, n), :] for c in range(3)]
            up = [DT * VISC - (0.5 * DT) * here[c] for c in range(3)]
            down = [DT * VISC + (0.5 * DT) * here[c] for c in range(3)]
            up[2] = up[2] * has_above
            down[2] = down[2] * has_below
            for c in range(3):
                window = jnp.concatenate(
                    [vbuf[c, z, pl.ds(prev, 8), :], here[c], vbuf[c, z, pl.ds(nxt, 8), :]], axis=0
                )
                total = (1.0 - 6.0 * DT * VISC) * here[c] + DT * force[pl.ds(c * ny + y0, n), :]
                total += up[0] * pltpu.roll(here[c], nx - 1, 1) + down[0] * pltpu.roll(here[c], 1, 1)
                total += up[1] * pltpu.roll(window, n + 15, 0)[8 : 8 + n]
                total += down[1] * pltpu.roll(window, 1, 0)[8 : 8 + n]
                total += up[2] * vbuf[c, above, pl.ds(y0, n), :]
                total += down[2] * vbuf[c, below, pl.ds(y0, n), :]
                obuf[c, z, pl.ds(y0, n), :] = total
            return 0

        lax.fori_loop(0, ny // 16, stencil, 0)
        pltpu.make_async_copy(obuf.at[:, z], p_hbm.at[:, z], out_sem.at[z]).start()
        return 0

    lax.fori_loop(0, layers, plane, 0)
    for z in range(layers):
        pltpu.make_async_copy(obuf.at[:, z], p_hbm.at[:, z], out_sem.at[z]).wait()


def spread_and_advance(own, near, moved, velocity):
    _, layers, ny, nx = velocity.shape
    both = 2 * own.shape[1]
    vmem = pl.BlockSpec(memory_space=pltpu.VMEM)
    hbm = pl.BlockSpec(memory_space=pl.ANY)
    flops = 2 * both * 3 * layers * ny * nx
    return pl.pallas_call(
        functools.partial(spread_kernel, layers, len(moved)),
        out_shape=jax.ShapeDtypeStruct(velocity.shape, jnp.float32),
        in_specs=[vmem] * (2 + len(moved)) + [hbm],
        out_specs=hbm,
        scratch_shapes=[
            pltpu.VMEM(velocity.shape, jnp.float32),
            pltpu.VMEM(velocity.shape, jnp.float32),
            pltpu.VMEM((3 * ny, nx), jnp.float32),
            pltpu.VMEM((3 * ny, both), jnp.bfloat16),
            pltpu.VMEM((both, nx), jnp.bfloat16),
            pltpu.VMEM((ny, both), jnp.float32),
            pltpu.VMEM((both, 8), jnp.float32),
            pltpu.VMEM((layers, 8, both), jnp.float32),
            pltpu.SemaphoreType.DMA,
            pltpu.SemaphoreType.DMA((layers,)),
        ],
        cost_estimate=pl.CostEstimate(
            flops=flops, bytes_accessed=8 * velocity.size, transcendentals=0
        ),
        name="spread_and_advance",
    )(own, near, *moved, velocity)


def edge_kernel(v_ref, p_ref, before_ref, after_ref, out_ref, *low_refs):
    side = pl.program_id(0)
    vz = v_ref[0, 0]

    @pl.when(side == 0)
    def _():
        down = DT * VISC + (0.5 * DT) * vz
        for c in range(3):
            new = p_ref[c, 0] + down * before_ref[c].astype(jnp.float32)
            out_ref[c, 0] = new
            if low_refs:
                low_refs[0][c] = new.astype(jnp.bfloat16)

    @pl.when(side == 1)
    def _():
        up = DT * VISC - (0.5 * DT) * vz
        for c in range(3):
            new = p_ref[c, 0] + up * after_ref[c].astype(jnp.float32)
            out_ref[c, 0] = new
            if low_refs:
                low_refs[1][c] = new.astype(jnp.bfloat16)


def finish_edges(velocity, partial, before, after, send):
    _, layers, ny, nx = velocity.shape
    yb = 64
    blocks = ny // yb
    wide = pl.BlockSpec((3, 1, yb, nx), lambda s, y: (0, s * (layers - 1), y, 0))
    head = pl.BlockSpec((3, yb, nx), lambda s, y: (0, jnp.where(s == 0, y, blocks - 1), 0))
    tail = pl.BlockSpec((3, yb, nx), lambda s, y: (0, jnp.where(s == 1, y, 0), 0))
    low = jax.ShapeDtypeStruct((3, ny, nx), jnp.bfloat16)
    return pl.pallas_call(
        edge_kernel,
        grid=(2, blocks),
        out_shape=[jax.ShapeDtypeStruct(partial.shape, jnp.float32)] + [low, low] * send,
        in_specs=[
            pl.BlockSpec((1, 1, yb, nx), lambda s, y: (2, s * (layers - 1), y, 0)),
            wide,
            head,
            tail,
        ],
        out_specs=[wide] + [head, tail] * send,
        input_output_aliases={1: 0},
        cost_estimate=pl.CostEstimate(
            flops=12 * ny * nx, bytes_accessed=50 * ny * nx, transcendentals=0
        ),
        name="finish_edges",
    )(velocity, partial, before, after)


def sample_kernel(layers, n_moved, *refs):
    own_ref, near_ref = refs[:2]
    moved = refs[2 : 2 + n_moved]
    v_hbm, own_out, near_out = refs[2 + n_moved : 5 + n_moved]
    vbuf, low, lhs, xtab, ytab, col, sem = refs[5 + n_moved :]
    ny, nx = vbuf.shape[2], vbuf.shape[3]
    both = xtab.shape[0]
    markers = both // 2

    copies = []
    for z in range(layers):
        copies.append(pltpu.make_async_copy(v_hbm.at[:, z], vbuf.at[:, z], sem.at[z]))
        copies[-1].start()

    offsets, cells, level, _ = joined(own_ref, near_ref, moved, layers)
    weights = weights_of(offsets)
    planes = plane_weights(level, [w[2:3] for w in weights], layers)
    rows = []
    for a in range(2):
        rows += [cells[a : a + 1].astype(jnp.float32)] + [w[a : a + 1] for w in weights]
    col[...] = columns_of(rows + planes)
    fill_xtable(xtab, col, 0, jnp.float32, nx, 64)
    fill_xtable(ytab, col, 5, jnp.float32, ny, 64)

    def lhs_body(i, _):
        r = pl.ds(i * 64, 64)
        y = ytab[r, :]
        cols = col[r, :]
        for z in range(layers):
            lhs[r, z * ny : (z + 1) * ny] = (cols[:, 10 + z : 11 + z] * y).astype(jnp.bfloat16)
        return 0

    lax.fori_loop(0, both // 64, lhs_body, 0)

    for z in range(layers):
        copies[z].wait()

        def low_body(i, _):
            r = pl.ds(i * 64, 64)
            for c in range(3):
                low[c, pl.ds(z * ny + i * 64, 64), :] = vbuf[c, z, r, :].astype(jnp.bfloat16)
            return 0

        lax.fori_loop(0, ny // 64, low_body, 0)

    for part, out, depth in ((0, own_out, layers * ny), (1, near_out, 3 * ny)):
        r = slice(part * markers, (part + 1) * markers)
        sums = []
        for c in range(3):
            lines = jnp.dot(
                lhs[r, :depth], low[c, :depth, :], preferred_element_type=jnp.float32
            )
            sums.append(jnp.sum(lines * xtab[r, :], axis=1, keepdims=True))
        zero = jnp.zeros((markers, 5), jnp.float32)
        out[...] = jnp.concatenate(sums + [zero], axis=1).T


def sample(own, near, moved, velocity):
    _, layers, ny, nx = velocity.shape
    markers = own.shape[1]
    both = 2 * markers
    vmem = pl.BlockSpec(memory_space=pltpu.VMEM)
    hbm = pl.BlockSpec(memory_space=pl.ANY)
    part = jax.ShapeDtypeStruct((8, markers), jnp.float32)
    return pl.pallas_call(
        functools.partial(sample_kernel, layers, len(moved)),
        out_shape=[part, part],
        in_specs=[vmem] * (2 + len(moved)) + [hbm],
        out_specs=[vmem, vmem],
        scratch_shapes=[
            pltpu.VMEM(velocity.shape, jnp.float32),
            pltpu.VMEM((3, layers * ny, nx), jnp.bfloat16),
            pltpu.VMEM((both, layers * ny), jnp.bfloat16),
            pltpu.VMEM((both, nx), jnp.float32),
            pltpu.VMEM((both, ny), jnp.float32),
            pltpu.VMEM((both, 16), jnp.float32),
            pltpu.SemaphoreType.DMA((layers,)),
        ],
        cost_estimate=pl.CostEstimate(
            flops=2 * both * 3 * layers * ny * nx,
            bytes_accessed=4 * velocity.size,
            transcendentals=0,
        ),
        name="sample",
    )(own, near, *moved, velocity)


def local(velocity, offsets, bases, targets, stiffness, active_block_count):
    layers = velocity.shape[1]
    markers = offsets.shape[1]
    living = (jnp.arange(markers, dtype=jnp.int32) // BLK < active_block_count[0]).astype(jnp.float32)
    level = bases[2] - lax.axis_index("gz") * layers
    own = jnp.concatenate(
        [
            offsets,
            bases[:2].astype(jnp.float32),
            level[None].astype(jnp.float32),
            targets,
            living[None],
            (living * stiffness)[None],
            jnp.zeros((ROWS - 11, markers), jnp.float32),
        ],
        axis=0,
    )
    near = shifted(own, 1)
    before = shifted(velocity[:, layers - 1].astype(jnp.bfloat16), 1)
    after = shifted(velocity[:, 0].astype(jnp.bfloat16), -1)
    moved = ()
    for step in range(STEPS):
        last = step == STEPS - 1
        partial = spread_and_advance(own, near, moved, velocity)
        done = finish_edges(velocity, partial, before, after, 0 if last else 1)
        velocity = done[0]
        if not last:
            before = shifted(done[2], 1)
            after = shifted(done[1], -1)
        own_part, near_part = sample(own, near, moved, velocity)
        back = shifted(near_part, -1)
        if not last:
            moved = (own_part, back, shifted(own_part, 1), near_part)
        offsets = offsets + DT * (living[None, :] * (own_part[:3] + back[:3]))
    return (velocity, offsets)


def solution(mesh):
    return jax.shard_map(
        local,
        mesh=mesh,
        in_specs=(
            P(None, "gz", None, None),
            P(None, "gz"),
            P(None, "gz"),
            P(None, "gz"),
            P("gz"),
            P("gz"),
        ),
        out_specs=(P(None, "gz", None, None), P(None, "gz")),
        check_vma=False,
    )
```

```python
import functools
import math

import jax
import jax.numpy as jnp
from jax import lax
from jax.experimental import pallas as pl
from jax.experimental.pallas import tpu as pltpu
from jax.sharding import PartitionSpec as P

BLK = 256
STEPS = 2
DT = 0.2
VISC = 0.3
TABLE = 128
ROWS = 16


def shifted(value, steps):
    count = lax.axis_size("gz")
    pairs = [(source, (source + steps) % count) for source in range(count)]
    return lax.ppermute(value, "gz", pairs)


def joined(own_ref, near_ref, moved, layers):
    halves = []
    for ref, pair in ((own_ref, moved[:2]), (near_ref, moved[2:])):
        rows = ref[...]
        offsets = rows[0:3]
        if pair:
            sampled = pair[0][0:3, :] + pair[1][0:3, :]
            offsets = offsets + DT * (rows[9:10] * sampled)
        level = rows[5:6] if ref is own_ref else rows[5:6] - float(layers)
        forces = rows[10:11] * (rows[6:9] - offsets)
        halves.append((offsets, rows[3:5].astype(jnp.int32), level.astype(jnp.int32), forces))
    return [jnp.concatenate(parts, axis=1) for parts in zip(*halves)]


def weights_of(offsets):
    angle = (0.5 * math.pi) * offsets
    c, s = jnp.cos(angle), jnp.sin(angle)
    return [0.25 * (1.0 + c), 0.25 * (1.0 + s), 0.25 * (1.0 - c), 0.25 * (1.0 - s)]


def banded(across, cell, weights, extent):
    apart = across - cell
    if extent & (extent - 1) == 0:
        apart = apart & (extent - 1)
    else:
        apart = jnp.where(apart < 0, apart + extent, apart)
    table = jnp.where(apart == 3, weights[3], 0.0)
    for j in (2, 1, 0):
        table = jnp.where(apart == j, weights[j], table)
    return table


def plane_weights(level, weights_z, layers):
    planes = []
    for z in range(layers):
        row = jnp.zeros(level.shape, jnp.float32)
        for j in range(4):
            row = jnp.where(level + j == z, weights_z[j], row)
        planes.append(row)
    return planes


def columns_of(rows):
    pad = -len(rows) % 8
    zero = jnp.zeros_like(rows[0])
    return jnp.concatenate(rows + [zero] * pad, axis=0).T


def fill_xtable(table_ref, col_ref, first, low, extent, chunk):
    def body(i, _):
        r = pl.ds(i * chunk, chunk)
        cols = col_ref[r, :]
        across = lax.broadcasted_iota(jnp.int32, (chunk, extent), 1)
        cell = cols[:, first : first + 1].astype(jnp.int32)
        ws = [cols[:, first + 1 + j : first + 2 + j] for j in range(4)]
        table_ref[r, :] = banded(across, cell, ws, extent).astype(low)
        return 0

    lax.fori_loop(0, table_ref.shape[0] // chunk, body, 0)


def spread_kernel(layers, n_moved, *refs):
    own_ref, near_ref = refs[:2]
    moved = refs[2 : 2 + n_moved]
    v_hbm, p_hbm, col = refs[2 + n_moved : 5 + n_moved]
    vbuf, obuf, force, lhs, xtab, ytab, rowg, in_sem, out_sem = refs[5 + n_moved :]
    ny, nx = vbuf.shape[2], vbuf.shape[3]
    both = xtab.shape[0]

    load = pltpu.make_async_copy(v_hbm, vbuf, in_sem)
    load.start()

    offsets, cells, level, forces = joined(own_ref, near_ref, moved, layers)
    weights = weights_of(offsets)
    planes = plane_weights(level, [w[2:3] for w in weights], layers)
    rows = []
    for a in range(2):
        rows += [cells[a : a + 1].astype(jnp.float32)] + [w[a : a + 1] for w in weights]
    col[...] = columns_of(rows + planes)
    for z in range(layers):
        rowg[z] = jnp.concatenate([forces * planes[z], jnp.zeros((5, both), jnp.float32)], axis=0)
    fill_xtable(xtab, col, 0, jnp.bfloat16, nx, TABLE)

    wy = [w[1:2] for w in weights]

    def ybody(i, _):
        across = lax.broadcasted_iota(jnp.int32, (32, both), 0) + i * 32
        ytab[pl.ds(i * 32, 32), :] = banded(across, cells[1:2], wy, ny)
        return 0

    lax.fori_loop(0, ny // 32, ybody, 0)
    load.wait()

    def plane(z, _):
        def lhs_body(i, _):
            y = ytab[pl.ds(i * 16, 16), :]
            for c in range(3):
                lhs[pl.ds(c * ny + i * 16, 16), :] = (rowg[z, c : c + 1, :] * y).astype(jnp.bfloat16)
            return 0

        lax.fori_loop(0, ny // 16, lhs_body, 0)
        force[...] = jnp.dot(lhs[...], xtab[...], preferred_element_type=jnp.float32)

        below = jnp.maximum(z - 1, 0)
        above = jnp.minimum(z + 1, layers - 1)
        has_below = jnp.where(z > 0, 1.0, 0.0)
        has_above = jnp.where(z < layers - 1, 1.0, 0.0)

        def stencil(i, _):
            n = 16
            y0 = i * n
            prev = jnp.where(i == 0, ny - 8, y0 - 8)
            nxt = jnp.where(y0 + n == ny, 0, y0 + n)
            here = [vbuf[c, z, pl.ds(y0, n), :] for c in range(3)]
            up = [DT * VISC - (0.5 * DT) * here[c] for c in range(3)]
            down = [DT * VISC + (0.5 * DT) * here[c] for c in range(3)]
            up[2] = up[2] * has_above
            down[2] = down[2] * has_below
            for c in range(3):
                window = jnp.concatenate(
                    [vbuf[c, z, pl.ds(prev, 8), :], here[c], vbuf[c, z, pl.ds(nxt, 8), :]], axis=0
                )
                total = (1.0 - 6.0 * DT * VISC) * here[c] + DT * force[pl.ds(c * ny + y0, n), :]
                total += up[0] * pltpu.roll(here[c], nx - 1, 1) + down[0] * pltpu.roll(here[c], 1, 1)
                total += up[1] * pltpu.roll(window, n + 15, 0)[8 : 8 + n]
                total += down[1] * pltpu.roll(window, 1, 0)[8 : 8 + n]
                total += up[2] * vbuf[c, above, pl.ds(y0, n), :]
                total += down[2] * vbuf[c, below, pl.ds(y0, n), :]
                obuf[c, z, pl.ds(y0, n), :] = total
            return 0

        lax.fori_loop(0, ny // 16, stencil, 0)
        pltpu.make_async_copy(obuf.at[:, z], p_hbm.at[:, z], out_sem.at[z]).start()
        return 0

    lax.fori_loop(0, layers, plane, 0)
    for z in range(layers):
        pltpu.make_async_copy(obuf.at[:, z], p_hbm.at[:, z], out_sem.at[z]).wait()


def spread_and_advance(own, near, moved, velocity):
    _, layers, ny, nx = velocity.shape
    both = 2 * own.shape[1]
    vmem = pl.BlockSpec(memory_space=pltpu.VMEM)
    hbm = pl.BlockSpec(memory_space=pl.ANY)
    flops = 2 * both * 3 * layers * ny * nx
    return pl.pallas_call(
        functools.partial(spread_kernel, layers, len(moved)),
        out_shape=[
            jax.ShapeDtypeStruct(velocity.shape, jnp.float32),
            jax.ShapeDtypeStruct((both, 16), jnp.float32),
        ],
        in_specs=[vmem] * (2 + len(moved)) + [hbm],
        out_specs=[hbm, vmem],
        scratch_shapes=[
            pltpu.VMEM(velocity.shape, jnp.float32),
            pltpu.VMEM(velocity.shape, jnp.float32),
            pltpu.VMEM((3 * ny, nx), jnp.float32),
            pltpu.VMEM((3 * ny, both), jnp.bfloat16),
            pltpu.VMEM((both, nx), jnp.bfloat16),
            pltpu.VMEM((ny, both), jnp.float32),
            pltpu.VMEM((layers, 8, both), jnp.float32),
            pltpu.SemaphoreType.DMA,
            pltpu.SemaphoreType.DMA((layers,)),
        ],
        cost_estimate=pl.CostEstimate(
            flops=flops, bytes_accessed=8 * velocity.size, transcendentals=0
        ),
        name="spread_and_advance",
    )(own, near, *moved, velocity)


def sample_kernel(layers, send, *refs):
    col, v_hbm, p_hbm, before_hbm, after_hbm, out_hbm, own_out, near_out = refs[:8]
    low_hbm = refs[8 : 8 + 2 * send]
    vbuf, vz, halo, low, lhs, xtab, sem, out_sem = refs[8 + 2 * send :]
    ny, nx = vbuf.shape[2], vbuf.shape[3]
    both = xtab.shape[0]
    markers = both // 2
    edges = ((0, before_hbm, 0.5 * DT), (layers - 1, after_hbm, -0.5 * DT))

    loads = []
    for side, (z, halo_hbm, _) in enumerate(edges):
        loads.append(pltpu.make_async_copy(p_hbm.at[:, z], vbuf.at[:, z], sem.at[z]))
        loads.append(pltpu.make_async_copy(v_hbm.at[2, z], vz.at[side], sem.at[layers + side]))
        loads.append(pltpu.make_async_copy(halo_hbm, halo.at[side], sem.at[layers + 2 + side]))
    for z in range(1, layers - 1):
        loads.append(pltpu.make_async_copy(p_hbm.at[:, z], vbuf.at[:, z], sem.at[z]))
    for load in loads:
        load.start()

    fill_xtable(xtab, col, 0, jnp.float32, nx, TABLE)

    def lhs_body(i, _):
        r = pl.ds(i * TABLE, TABLE)
        cols = col[r, :]
        across = lax.broadcasted_iota(jnp.int32, (TABLE, ny), 1)
        cell = cols[:, 5:6].astype(jnp.int32)
        y = banded(across, cell, [cols[:, 6 + j : 7 + j] for j in range(4)], ny)
        for z in range(layers):
            lhs[r, z * ny : (z + 1) * ny] = (cols[:, 10 + z : 11 + z] * y).astype(jnp.bfloat16)
        return 0

    lax.fori_loop(0, both // TABLE, lhs_body, 0)
    for load in loads:
        load.wait()

    stores = []
    for side, (z, _, sign) in enumerate(edges):

        def edge_body(i, _):
            r = pl.ds(i * 32, 32)
            factor = DT * VISC + sign * vz[side, r, :]
            for c in range(3):
                new = vbuf[c, z, r, :] + factor * halo[side, c, r, :].astype(jnp.float32)
                vbuf[c, z, r, :] = new
                low[c, pl.ds(z * ny + i * 32, 32), :] = new.astype(jnp.bfloat16)
            return 0

        lax.fori_loop(0, ny // 32, edge_body, 0)
        stores.append(pltpu.make_async_copy(vbuf.at[:, z], out_hbm.at[:, z], out_sem.at[side]))
        if send:
            stores.append(
                pltpu.make_async_copy(
                    low.at[:, z * ny : (z + 1) * ny], low_hbm[side], out_sem.at[2 + side]
                )
            )
    for store in stores:
        store.start()

    def low_body(i, _):
        r = pl.ds(i * 32, 32)
        for z in range(1, layers - 1):
            for c in range(3):
                low[c, pl.ds(z * ny + i * 32, 32), :] = vbuf[c, z, r, :].astype(jnp.bfloat16)
        return 0

    lax.fori_loop(0, ny // 32, low_body, 0)

    for part, out, depth in ((0, own_out, layers * ny), (1, near_out, 3 * ny)):
        r = slice(part * markers, (part + 1) * markers)
        sums = []
        for c in range(3):
            lines = jnp.dot(
                lhs[r, :depth], low[c, :depth, :], preferred_element_type=jnp.float32
            )
            sums.append(jnp.sum(lines * xtab[r, :], axis=1, keepdims=True))
        zero = jnp.zeros((markers, 5), jnp.float32)
        out[...] = jnp.concatenate(sums + [zero], axis=1).T
    for store in stores:
        store.wait()


def finish_and_sample(col, velocity, partial, before, after, send):
    _, layers, ny, nx = velocity.shape
    both = col.shape[0]
    markers = both // 2
    vmem = pl.BlockSpec(memory_space=pltpu.VMEM)
    hbm = pl.BlockSpec(memory_space=pl.ANY)
    part = jax.ShapeDtypeStruct((8, markers), jnp.float32)
    low = jax.ShapeDtypeStruct((3, ny, nx), jnp.bfloat16)
    return pl.pallas_call(
        functools.partial(sample_kernel, layers, send),
        out_shape=[jax.ShapeDtypeStruct(velocity.shape, jnp.float32), part, part] + [low, low] * send,
        in_specs=[vmem] + [hbm] * 4,
        out_specs=[hbm, vmem, vmem] + [hbm, hbm] * send,
        input_output_aliases={2: 0},
        scratch_shapes=[
            pltpu.VMEM(velocity.shape, jnp.float32),
            pltpu.VMEM((2, ny, nx), jnp.float32),
            pltpu.VMEM((2, 3, ny, nx), jnp.bfloat16),
            pltpu.VMEM((3, layers * ny, nx), jnp.bfloat16),
            pltpu.VMEM((both, layers * ny), jnp.bfloat16),
            pltpu.VMEM((both, nx), jnp.float32),
            pltpu.SemaphoreType.DMA((layers + 4,)),
            pltpu.SemaphoreType.DMA((4,)),
        ],
        cost_estimate=pl.CostEstimate(
            flops=2 * both * 3 * layers * ny * nx,
            bytes_accessed=4 * velocity.size,
            transcendentals=0,
        ),
        name="finish_and_sample",
    )(col, velocity, partial, before, after)


def local(velocity, offsets, bases, targets, stiffness, active_block_count):
    layers = velocity.shape[1]
    markers = offsets.shape[1]
    living = (jnp.arange(markers, dtype=jnp.int32) // BLK < active_block_count[0]).astype(jnp.float32)
    level = bases[2] - lax.axis_index("gz") * layers
    own = jnp.concatenate(
        [
            offsets,
            bases[:2].astype(jnp.float32),
            level[None].astype(jnp.float32),
            targets,
            living[None],
            (living * stiffness)[None],
            jnp.zeros((ROWS - 11, markers), jnp.float32),
        ],
        axis=0,
    )
    first = velocity[:, 0].astype(jnp.bfloat16)
    final = velocity[:, layers - 1].astype(jnp.bfloat16)
    near = shifted(own, 1)
    moved = ()
    for step in range(STEPS):
        last = step == STEPS - 1
        if moved:
            first, final, *moved = lax.optimization_barrier((first, final, *moved))
        else:
            first, final, near = lax.optimization_barrier((first, final, near))
        before = shifted(final, 1)
        after = shifted(first, -1)
        partial, col = spread_and_advance(own, near, moved, velocity)
        velocity, own_part, near_part, *low = finish_and_sample(
            col, velocity, partial, before, after, 0 if last else 1
        )
        back = shifted(near_part, -1)
        if not last:
            first, final = low
            moved = (own_part, back, shifted(own_part, 1), near_part)
        offsets = offsets + DT * (living[None, :] * (own_part[:3] + back[:3]))
    return (velocity, offsets)


def solution(mesh):
    return jax.shard_map(
        local,
        mesh=mesh,
        in_specs=(
            P(None, "gz", None, None),
            P(None, "gz"),
            P(None, "gz"),
            P(None, "gz"),
            P("gz"),
            P("gz"),
        ),
        out_specs=(P(None, "gz", None, None), P(None, "gz")),
        check_vma=False,
    )
```

```python
import functools
import math

import jax
import jax.numpy as jnp
from jax import lax
from jax.experimental import pallas as pl
from jax.experimental.pallas import tpu as pltpu
from jax.sharding import PartitionSpec as P

BLK = 256
STEPS = 2
DT = 0.2
VISC = 0.3
TABLE = 128
ROWS = 16


def shifted(value, steps):
    count = lax.axis_size("gz")
    pairs = [(source, (source + steps) % count) for source in range(count)]
    return lax.ppermute(value, "gz", pairs)


def joined(own_ref, near_ref, moved, layers):
    halves = []
    for ref, pair in ((own_ref, moved[:2]), (near_ref, moved[2:])):
        rows = ref[...]
        offsets = rows[0:3]
        if pair:
            sampled = pair[0][0:3, :] + pair[1][0:3, :]
            offsets = offsets + DT * (rows[9:10] * sampled)
        level = rows[5:6] if ref is own_ref else rows[5:6] - float(layers)
        forces = rows[10:11] * (rows[6:9] - offsets)
        halves.append((offsets, rows[3:5].astype(jnp.int32), level.astype(jnp.int32), forces))
    return [jnp.concatenate(parts, axis=1) for parts in zip(*halves)]


def weights_of(offsets):
    angle = (0.5 * math.pi) * offsets
    c, s = jnp.cos(angle), jnp.sin(angle)
    return [0.25 * (1.0 + c), 0.25 * (1.0 + s), 0.25 * (1.0 - c), 0.25 * (1.0 - s)]


def banded(across, cell, weights, extent):
    apart = across - cell
    if extent & (extent - 1) == 0:
        apart = apart & (extent - 1)
    else:
        apart = jnp.where(apart < 0, apart + extent, apart)
    table = jnp.where(apart == 3, weights[3], 0.0)
    for j in (2, 1, 0):
        table = jnp.where(apart == j, weights[j], table)
    return table


def plane_weights(level, weights_z, layers):
    planes = []
    for z in range(layers):
        row = jnp.zeros(level.shape, jnp.float32)
        for j in range(4):
            row = jnp.where(level + j == z, weights_z[j], row)
        planes.append(row)
    return planes


def columns_of(rows):
    pad = -len(rows) % 8
    zero = jnp.zeros_like(rows[0])
    return jnp.concatenate(rows + [zero] * pad, axis=0).T


def fill_xtable(table_ref, col_ref, first, low, extent, chunk):
    def body(i, _):
        r = pl.ds(i * chunk, chunk)
        cols = col_ref[r, :]
        across = lax.broadcasted_iota(jnp.int32, (chunk, extent), 1)
        cell = cols[:, first : first + 1].astype(jnp.int32)
        ws = [cols[:, first + 1 + j : first + 2 + j] for j in range(4)]
        table_ref[r, :] = banded(across, cell, ws, extent).astype(low)
        return 0

    lax.fori_loop(0, table_ref.shape[0] // chunk, body, 0)


def stencil_kernel(v_hbm, p_hbm, vbuf, obuf, in_sem, out_sem):
    layers, ny, nx = vbuf.shape[1:]

    def load(z):
        return pltpu.make_async_copy(v_hbm.at[:, z], vbuf.at[:, z], in_sem.at[z])

    def store(z):
        return pltpu.make_async_copy(obuf.at[:, z], p_hbm.at[:, z], out_sem.at[z])

    for z in range(layers):
        load(z).start()
    load(0).wait()

    def plane(z, _):
        @pl.when(z < layers - 1)
        def _():
            load(z + 1).wait()

        below = jnp.maximum(z - 1, 0)
        above = jnp.minimum(z + 1, layers - 1)
        has_below = jnp.where(z > 0, 1.0, 0.0)
        has_above = jnp.where(z < layers - 1, 1.0, 0.0)

        def stencil(i, _):
            n = 8
            y0 = i * n
            prev = jnp.where(i == 0, ny - 8, y0 - 8)
            nxt = jnp.where(y0 + n == ny, 0, y0 + n)
            here = [vbuf[c, z, pl.ds(y0, n), :] for c in range(3)]
            up = [DT * VISC - (0.5 * DT) * here[c] for c in range(3)]
            down = [DT * VISC + (0.5 * DT) * here[c] for c in range(3)]
            up[2] = up[2] * has_above
            down[2] = down[2] * has_below
            for c in range(3):
                window = jnp.concatenate(
                    [vbuf[c, z, pl.ds(prev, 8), :], here[c], vbuf[c, z, pl.ds(nxt, 8), :]], axis=0
                )
                total = (1.0 - 6.0 * DT * VISC) * here[c]
                total += up[0] * pltpu.roll(here[c], nx - 1, 1) + down[0] * pltpu.roll(here[c], 1, 1)
                total += up[1] * pltpu.roll(window, n + 15, 0)[8 : 8 + n]
                total += down[1] * pltpu.roll(window, 1, 0)[8 : 8 + n]
                total += up[2] * vbuf[c, above, pl.ds(y0, n), :]
                total += down[2] * vbuf[c, below, pl.ds(y0, n), :]
                obuf[c, z, pl.ds(y0, n), :] = total
            return 0

        lax.fori_loop(0, ny // 8, stencil, 0, unroll=2)
        store(z).start()
        return 0

    lax.fori_loop(0, layers, plane, 0)
    for z in range(layers):
        store(z).wait()


def stencil_terms(velocity):
    layers = velocity.shape[1]
    hbm = pl.BlockSpec(memory_space=pl.ANY)
    return pl.pallas_call(
        stencil_kernel,
        out_shape=jax.ShapeDtypeStruct(velocity.shape, jnp.float32),
        in_specs=[hbm],
        out_specs=hbm,
        scratch_shapes=[
            pltpu.VMEM(velocity.shape, jnp.float32),
            pltpu.VMEM(velocity.shape, jnp.float32),
            pltpu.SemaphoreType.DMA((layers,)),
            pltpu.SemaphoreType.DMA((layers,)),
        ],
        cost_estimate=pl.CostEstimate(
            flops=6000 * velocity.size, bytes_accessed=8 * velocity.size, transcendentals=0
        ),
        name="stencil_terms",
    )(velocity)


def spread_kernel(layers, n_moved, *refs):
    own_ref, near_ref = refs[:2]
    moved = refs[2 : 2 + n_moved]
    v_hbm, p_hbm, col = refs[2 + n_moved : 5 + n_moved]
    obuf, force, lhs, xtab, ytab, rowg, in_sem, out_sem = refs[5 + n_moved :]
    ny, nx = obuf.shape[2], obuf.shape[3]
    both = xtab.shape[0]

    load = pltpu.make_async_copy(v_hbm, obuf, in_sem)
    load.start()

    offsets, cells, level, forces = joined(own_ref, near_ref, moved, layers)
    weights = weights_of(offsets)
    planes = plane_weights(level, [w[2:3] for w in weights], layers)
    rows = []
    for a in range(2):
        rows += [cells[a : a + 1].astype(jnp.float32)] + [w[a : a + 1] for w in weights]
    col[...] = columns_of(rows + planes)
    for z in range(layers):
        rowg[z] = jnp.concatenate([forces * planes[z], jnp.zeros((5, both), jnp.float32)], axis=0)
    fill_xtable(xtab, col, 0, jnp.bfloat16, nx, TABLE)

    wy = [w[1:2] for w in weights]

    def ybody(i, _):
        across = lax.broadcasted_iota(jnp.int32, (32, both), 0) + i * 32
        ytab[pl.ds(i * 32, 32), :] = banded(across, cells[1:2], wy, ny)
        return 0

    lax.fori_loop(0, ny // 32, ybody, 0)
    load.wait()

    def plane(z, _):
        def lhs_body(i, _):
            y = ytab[pl.ds(i * 16, 16), :]
            for c in range(3):
                lhs[pl.ds(c * ny + i * 16, 16), :] = (rowg[z, c : c + 1, :] * y).astype(jnp.bfloat16)
            return 0

        lax.fori_loop(0, ny // 16, lhs_body, 0)
        force[...] = jnp.dot(lhs[...], xtab[...], preferred_element_type=jnp.float32)

        def add(i, _):
            r = pl.ds(i * 32, 32)
            for c in range(3):
                obuf[c, z, r, :] += DT * force[pl.ds(c * ny + i * 32, 32), :]
            return 0

        lax.fori_loop(0, ny // 32, add, 0)
        pltpu.make_async_copy(obuf.at[:, z], p_hbm.at[:, z], out_sem.at[z]).start()
        return 0

    lax.fori_loop(0, layers, plane, 0)
    for z in range(layers):
        pltpu.make_async_copy(obuf.at[:, z], p_hbm.at[:, z], out_sem.at[z]).wait()


def add_forcing(own, near, moved, velocity):
    _, layers, ny, nx = velocity.shape
    both = 2 * own.shape[1]
    vmem = pl.BlockSpec(memory_space=pltpu.VMEM)
    hbm = pl.BlockSpec(memory_space=pl.ANY)
    flops = 2 * both * 3 * layers * ny * nx
    return pl.pallas_call(
        functools.partial(spread_kernel, layers, len(moved)),
        out_shape=[
            jax.ShapeDtypeStruct(velocity.shape, jnp.float32),
            jax.ShapeDtypeStruct((both, 16), jnp.float32),
        ],
        in_specs=[vmem] * (2 + len(moved)) + [hbm],
        out_specs=[hbm, vmem],
        input_output_aliases={2 + len(moved): 0},
        scratch_shapes=[
            pltpu.VMEM(velocity.shape, jnp.float32),
            pltpu.VMEM((3 * ny, nx), jnp.float32),
            pltpu.VMEM((3 * ny, both), jnp.bfloat16),
            pltpu.VMEM((both, nx), jnp.bfloat16),
            pltpu.VMEM((ny, both), jnp.float32),
            pltpu.VMEM((layers, 8, both), jnp.float32),
            pltpu.SemaphoreType.DMA,
            pltpu.SemaphoreType.DMA((layers,)),
        ],
        cost_estimate=pl.CostEstimate(
            flops=flops, bytes_accessed=8 * velocity.size, transcendentals=0
        ),
        name="add_forcing",
    )(own, near, *moved, velocity)


def sample_kernel(layers, send, *refs):
    col, v_hbm, p_hbm, before_hbm, after_hbm, out_hbm, own_out, near_out = refs[:8]
    low_hbm = refs[8 : 8 + 2 * send]
    vbuf, vz, halo, low, lhs, xtab, sem, out_sem = refs[8 + 2 * send :]
    ny, nx = vbuf.shape[2], vbuf.shape[3]
    both = xtab.shape[0]
    markers = both // 2
    edges = ((0, before_hbm, 0.5 * DT), (layers - 1, after_hbm, -0.5 * DT))

    loads = []
    for side, (z, halo_hbm, _) in enumerate(edges):
        loads.append(pltpu.make_async_copy(p_hbm.at[:, z], vbuf.at[:, z], sem.at[z]))
        loads.append(pltpu.make_async_copy(v_hbm.at[2, z], vz.at[side], sem.at[layers + side]))
        loads.append(pltpu.make_async_copy(halo_hbm, halo.at[side], sem.at[layers + 2 + side]))
    for z in range(1, layers - 1):
        loads.append(pltpu.make_async_copy(p_hbm.at[:, z], vbuf.at[:, z], sem.at[z]))
    for load in loads:
        load.start()

    fill_xtable(xtab, col, 0, jnp.float32, nx, TABLE)

    def lhs_body(i, _):
        r = pl.ds(i * TABLE, TABLE)
        cols = col[r, :]
        across = lax.broadcasted_iota(jnp.int32, (TABLE, ny), 1)
        cell = cols[:, 5:6].astype(jnp.int32)
        y = banded(across, cell, [cols[:, 6 + j : 7 + j] for j in range(4)], ny)
        for z in range(layers):
            lhs[r, z * ny : (z + 1) * ny] = (cols[:, 10 + z : 11 + z] * y).astype(jnp.bfloat16)
        return 0

    lax.fori_loop(0, both // TABLE, lhs_body, 0)
    for load in loads:
        load.wait()

    stores = []
    for side, (z, _, sign) in enumerate(edges):

        def edge_body(i, _):
            r = pl.ds(i * 32, 32)
            factor = DT * VISC + sign * vz[side, r, :]
            for c in range(3):
                new = vbuf[c, z, r, :] + factor * halo[side, c, r, :].astype(jnp.float32)
                vbuf[c, z, r, :] = new
                low[c, pl.ds(z * ny + i * 32, 32), :] = new.astype(jnp.bfloat16)
            return 0

        lax.fori_loop(0, ny // 32, edge_body, 0)
        stores.append(pltpu.make_async_copy(vbuf.at[:, z], out_hbm.at[:, z], out_sem.at[side]))
        if send:
            stores.append(
                pltpu.make_async_copy(
                    low.at[:, z * ny : (z + 1) * ny], low_hbm[side], out_sem.at[2 + side]
                )
            )
    for store in stores:
        store.start()

    def low_body(i, _):
        r = pl.ds(i * 32, 32)
        for z in range(1, layers - 1):
            for c in range(3):
                low[c, pl.ds(z * ny + i * 32, 32), :] = vbuf[c, z, r, :].astype(jnp.bfloat16)
        return 0

    lax.fori_loop(0, ny // 32, low_body, 0)

    for part, out, depth in ((0, own_out, layers * ny), (1, near_out, 3 * ny)):
        r = slice(part * markers, (part + 1) * markers)
        sums = []
        for c in range(3):
            lines = jnp.dot(
                lhs[r, :depth], low[c, :depth, :], preferred_element_type=jnp.float32
            )
            sums.append(jnp.sum(lines * xtab[r, :], axis=1, keepdims=True))
        zero = jnp.zeros((markers, 5), jnp.float32)
        out[...] = jnp.concatenate(sums + [zero], axis=1).T
    for store in stores:
        store.wait()


def finish_and_sample(col, velocity, partial, before, after, send):
    _, layers, ny, nx = velocity.shape
    both = col.shape[0]
    markers = both // 2
    vmem = pl.BlockSpec(memory_space=pltpu.VMEM)
    hbm = pl.BlockSpec(memory_space=pl.ANY)
    part = jax.ShapeDtypeStruct((8, markers), jnp.float32)
    low = jax.ShapeDtypeStruct((3, ny, nx), jnp.bfloat16)
    return pl.pallas_call(
        functools.partial(sample_kernel, layers, send),
        out_shape=[jax.ShapeDtypeStruct(velocity.shape, jnp.float32), part, part] + [low, low] * send,
        in_specs=[vmem] + [hbm] * 4,
        out_specs=[hbm, vmem, vmem] + [hbm, hbm] * send,
        input_output_aliases={2: 0},
        scratch_shapes=[
            pltpu.VMEM(velocity.shape, jnp.float32),
            pltpu.VMEM((2, ny, nx), jnp.float32),
            pltpu.VMEM((2, 3, ny, nx), jnp.bfloat16),
            pltpu.VMEM((3, layers * ny, nx), jnp.bfloat16),
            pltpu.VMEM((both, layers * ny), jnp.bfloat16),
            pltpu.VMEM((both, nx), jnp.float32),
            pltpu.SemaphoreType.DMA((layers + 4,)),
            pltpu.SemaphoreType.DMA((4,)),
        ],
        cost_estimate=pl.CostEstimate(
            flops=2 * both * 3 * layers * ny * nx,
            bytes_accessed=4 * velocity.size,
            transcendentals=0,
        ),
        name="finish_and_sample",
    )(col, velocity, partial, before, after)


def local(velocity, offsets, bases, targets, stiffness, active_block_count):
    layers = velocity.shape[1]
    markers = offsets.shape[1]
    living = (jnp.arange(markers, dtype=jnp.int32) // BLK < active_block_count[0]).astype(jnp.float32)
    level = bases[2] - lax.axis_index("gz") * layers
    own = jnp.concatenate(
        [
            offsets,
            bases[:2].astype(jnp.float32),
            level[None].astype(jnp.float32),
            targets,
            living[None],
            (living * stiffness)[None],
            jnp.zeros((ROWS - 11, markers), jnp.float32),
        ],
        axis=0,
    )
    first = velocity[:, 0].astype(jnp.bfloat16)
    final = velocity[:, layers - 1].astype(jnp.bfloat16)
    own, first, final = lax.optimization_barrier((own, first, final))
    near = shifted(own, 1)
    moved = ()
    for step in range(STEPS):
        last = step == STEPS - 1
        before = shifted(final, 1)
        after = shifted(first, -1)
        partial = stencil_terms(velocity)
        partial, col = add_forcing(own, near, moved, partial)
        velocity, own_part, near_part, *low = finish_and_sample(
            col, velocity, partial, before, after, 0 if last else 1
        )
        back = shifted(near_part, -1)
        if not last:
            first, final = low
            moved = (own_part, back, shifted(own_part, 1), near_part)
        offsets = offsets + DT * (living[None, :] * (own_part[:3] + back[:3]))
    return (velocity, offsets)


def solution(mesh):
    return jax.shard_map(
        local,
        mesh=mesh,
        in_specs=(
            P(None, "gz", None, None),
            P(None, "gz"),
            P(None, "gz"),
            P(None, "gz"),
            P("gz"),
            P("gz"),
        ),
        out_specs=(P(None, "gz", None, None), P(None, "gz")),
        check_vma=False,
    )
```
